32 devices in a mesh: aln: 4 (over y, x), rows: 8 (over z, core).
Axes of the slice: x: 2, y: 2, z: 4, core: 2. Of those that a mesh axis runs over, the one named last changes fastest.
Arguments:
- sequence_stack: bfloat16 [32, 8, 768], P(('aln', 'rows')), parts along dimension 0, may hold values from -6 to 6
- protein_spans: int32 [4], P('aln'), parts along dimension 0, may hold values from 1 to 8
- twofold_contacts: bfloat16 [32, 8, 128], P(('aln', 'rows')), parts along dimension 0, may hold values from -6 to 6
- horizontal_projection_triple: bfloat16 [768, 2304], P(None, 'rows'), may hold values from -0.21875 to 0.21875
- horizontal_projection_out: bfloat16 [768, 768], P(None, 'rows'), may hold values from -0.21875 to 0.21875
- vertical_projection_triple: bfloat16 [768, 2304], P(None, 'rows'), may hold values from -0.21875 to 0.21875
- vertical_projection_out: bfloat16 [768, 768], P(None, 'rows'), may hold values from -0.21875 to 0.21875
- contact_logit_offsets: bfloat16 [128, 12], replicated, may hold values from -0.5 to 0.5
- contact_projection_weights: bfloat16 [12, 128], replicated, may hold values from -1.75 to 1.75
Outputs:
- alignment_output: bfloat16 [32, 8, 768], P('aln', 'rows'), parts along dimension 0
- pair_feature_output: bfloat16 [32, 8, 128], P(('aln', 'rows')), parts along dimension 0
The draws below stay inside these ranges and needn't reach their ends.
There are 4 independent parts, one for each index of `aln`. The reference program is written for one: setup_inputs(seed, part) draws one part's arguments, and reference() takes and returns one part's arrays. A program takes and returns all parts, laid end to end along the dimension named above; an argument that names none is the same for every part. Nothing has to cross between parts.
All inputs are finite; a program needn't handle non-finite values.
Results may differ from the reference program's by a relative error of at most 0.0075.
Values may be sent and summed in bfloat16 or wider, within the bound.
A program may use at most 64 MiB of HBM per device.

```python
import jax
import jax.numpy as jnp
from jax import lax

D = 768
H = 12
P_SIZE = 128
R = 8
L = 8


def draw_sequence_stack(key, part):
    first = jax.random.fold_in(jax.random.fold_in(key, 11), 0)
    base = jnp.clip(jax.random.normal(first, (R, L, D), jnp.float32), -6.0, 6.0)
    return base.astype(jnp.bfloat16)


def levels(rng, dims, shards, least, high):
    loudness, own = 1.0, jax.random.fold_in(rng, 6)
    for axis_at, blocks in shards:
        heights = jnp.exp(jax.random.uniform(jax.random.fold_in(own, axis_at), (blocks,), jnp.float32, least / len(shards), high / len(shards)))
        loudness = loudness * jnp.repeat(heights, dims[axis_at] // blocks).reshape([-1 if axis == axis_at else 1 for axis in range(len(dims))])
    return loudness


def bell_draw(stream_key, extent, width, most, pieces=(), held_as=jnp.bfloat16):
    drawn = width * jax.random.normal(stream_key, extent, jnp.float32)
    if pieces:
        drawn = drawn * levels(stream_key, extent, pieces, -0.22, 0.18)
    return jnp.clip(drawn, -most, most).astype(held_as)


def setup_inputs(seed: int = 0, part: int = 0) -> dict:
    key_of = jax.random.split(jax.random.key(seed), 10)
    part_keys = jax.random.split(jax.random.fold_in(key_of[9], part), 10)
    return {
        "sequence_stack": draw_sequence_stack(jax.random.fold_in(jax.random.fold_in(key_of[9], part), 71), part),
        "protein_spans": jax.random.randint(part_keys[1], (1,), 1, L + 1).astype(jnp.int32),
        "twofold_contacts": bell_draw(part_keys[2], (L, L, P_SIZE), 1.0, 6.0, ((0, 8),)),
        "horizontal_projection_triple": bell_draw(key_of[3], (D, 3 * D), D ** -0.5, 0.21875, ((1, 8),)),
        "horizontal_projection_out": bell_draw(key_of[4], (D, D), D ** -0.5, 0.21875, ((1, 8),)),
        "vertical_projection_triple": bell_draw(key_of[5], (D, 3 * D), D ** -0.5, 0.21875, ((1, 8),)),
        "vertical_projection_out": bell_draw(key_of[6], (D, D), D ** -0.5, 0.21875, ((1, 8),)),
        "contact_logit_offsets": bell_draw(key_of[7], (P_SIZE, H), P_SIZE ** -0.5, 0.5),
        "contact_projection_weights": bell_draw(key_of[8], (H, P_SIZE), H ** -0.5, 1.75),
    }


def normalize(incoming_sequence_stack):
    center = lax.optimization_barrier(jnp.mean(incoming_sequence_stack, axis=-1, keepdims=True))
    spread = lax.optimization_barrier(jnp.mean(jnp.square(incoming_sequence_stack - center), axis=-1, keepdims=True))
    return (incoming_sequence_stack - center) * lax.rsqrt(spread + 1e-05)

def project_three(normed, weights, hidden_channel_size, head_count, shape_rows, shape_res):
    head_dim = hidden_channel_size // head_count
    packed = jnp.dot(normed, weights, preferred_element_type=jnp.float32)
    queries = (packed[:, :hidden_channel_size] * head_dim ** (-0.5)).astype(jnp.bfloat16)
    key_rows = packed[:, hidden_channel_size:2 * hidden_channel_size].astype(jnp.bfloat16)
    value_rows = packed[:, 2 * hidden_channel_size:].astype(jnp.bfloat16)
    input_dimensions = (shape_rows, shape_res, head_count, head_dim)
    return (queries.reshape(input_dimensions), key_rows.reshape(input_dimensions), value_rows.reshape(input_dimensions))

def reference(sequence_stack, protein_spans, twofold_contacts, horizontal_projection_triple, horizontal_projection_out, vertical_projection_triple, vertical_projection_out, contact_logit_offsets, contact_projection_weights):
    overall_sequence_number, sequence_positions, hidden_channel_size = sequence_stack.shape
    head_count = contact_logit_offsets.shape[1]
    channels = contact_logit_offsets.shape[0]
    incoming_sequence_stack = sequence_stack.astype(jnp.float32)
    normed = normalize(incoming_sequence_stack).astype(jnp.bfloat16).reshape(-1, hidden_channel_size)
    queries, key_rows, value_rows = project_three(normed, horizontal_projection_triple, hidden_channel_size, head_count, overall_sequence_number, sequence_positions)
    tied = jnp.einsum('rihe,rjhe->hij', queries.astype(jnp.float32), key_rows.astype(jnp.float32))
    bias_all = jnp.dot(twofold_contacts.reshape(-1, channels), contact_logit_offsets, preferred_element_type=jnp.float32)
    bias_all = bias_all.reshape(sequence_positions, sequence_positions, head_count).transpose(2, 0, 1)
    scores = tied * float(overall_sequence_number) ** (-0.5) + bias_all
    flat_scores = scores.astype(jnp.bfloat16).transpose(1, 2, 0).reshape(-1, head_count)
    pair_feature_output = (twofold_contacts.astype(jnp.float32) + jnp.dot(flat_scores, contact_projection_weights, preferred_element_type=jnp.float32).reshape(sequence_positions, sequence_positions, channels)).astype(jnp.bfloat16)
    key_valid = jnp.arange(sequence_positions, dtype=jnp.int32) < protein_spans[0]
    row_probs = jax.nn.softmax(jnp.where(key_valid[None, None, :], scores, -1e+30), axis=-1).astype(jnp.bfloat16)
    blended = jnp.einsum('hij,rjhe->rihe', row_probs.astype(jnp.float32), value_rows.astype(jnp.float32))
    blended = blended.astype(jnp.bfloat16).reshape(-1, hidden_channel_size)
    updated_alignment = (incoming_sequence_stack + jnp.dot(blended, horizontal_projection_out, preferred_element_type=jnp.float32).reshape(overall_sequence_number, sequence_positions, hidden_channel_size)).astype(jnp.bfloat16)
    col_normed = normalize(updated_alignment.astype(jnp.float32)).astype(jnp.bfloat16).reshape(-1, hidden_channel_size)
    col_queries, col_keys, col_values = project_three(col_normed, vertical_projection_triple, hidden_channel_size, head_count, overall_sequence_number, sequence_positions)

    def one_head(head):
        query_head = col_queries[:, :, head, :].astype(jnp.float32)
        key_head = col_keys[:, :, head, :].astype(jnp.float32)
        value_head = col_values[:, :, head, :].astype(jnp.float32)
        logits = jnp.einsum('ale,ble->lab', query_head, key_head)
        col_probs = jax.nn.softmax(logits, axis=-1).astype(jnp.bfloat16)
        return jnp.einsum('lab,ble->ale', col_probs.astype(jnp.float32), value_head)
    per_head = lax.map(one_head, jnp.arange(head_count, dtype=jnp.int32))
    column_mixed_output = per_head.transpose(1, 2, 0, 3).astype(jnp.bfloat16).reshape(-1, hidden_channel_size)
    alignment_output = (updated_alignment.astype(jnp.float32) + jnp.dot(column_mixed_output, vertical_projection_out, preferred_element_type=jnp.float32).reshape(overall_sequence_number, sequence_positions, hidden_channel_size)).astype(jnp.bfloat16)
    return (alignment_output, pair_feature_output)
```

```python
import functools

import jax
import jax.numpy as jnp
from jax import lax
from jax.experimental import pallas as pl
from jax.experimental.pallas import tpu as pltpu
from jax.sharding import PartitionSpec as P


def normalize(incoming_sequence_stack):
    center = jnp.mean(incoming_sequence_stack, axis=-1, keepdims=True)
    spread = jnp.mean(jnp.square(incoming_sequence_stack - center), axis=-1, keepdims=True)
    return (incoming_sequence_stack - center) * lax.rsqrt(spread + 1e-05)


def split_three(packed, hidden_channel_size, head_count, shape_rows, shape_res):
    head_dim = hidden_channel_size // head_count
    queries = (packed[:, :hidden_channel_size] * head_dim ** (-0.5)).astype(jnp.bfloat16)
    key_rows = packed[:, hidden_channel_size : 2 * hidden_channel_size].astype(jnp.bfloat16)
    value_rows = packed[:, 2 * hidden_channel_size :].astype(jnp.bfloat16)
    input_dimensions = (shape_rows, shape_res, head_count, head_dim)
    return (
        queries.reshape(input_dimensions),
        key_rows.reshape(input_dimensions),
        value_rows.reshape(input_dimensions),
    )


def masked_softmax(scores, protein_spans):
    key_valid = lax.broadcasted_iota(jnp.int32, (1, 1, scores.shape[2]), 2) < protein_spans[0]
    return jax.nn.softmax(jnp.where(key_valid, scores, -1e30), axis=-1).astype(jnp.bfloat16)


def per_device(
    sequence_stack,
    protein_spans,
    twofold_contacts,
    horizontal_projection_triple,
    horizontal_projection_out,
    vertical_projection_triple,
    vertical_projection_out,
    contact_logit_offsets,
    contact_projection_weights,
):
    sequences_per_shard, sequence_positions, hidden_channel_size = sequence_stack.shape
    parties = lax.axis_size("rows")
    overall_sequence_number = sequences_per_shard * parties
    residue_portion = sequence_positions // parties
    head_count = contact_logit_offsets.shape[1]
    channels = contact_logit_offsets.shape[0]
    scale_rows = float(overall_sequence_number) ** (-0.5)
    incoming_sequence_stack = sequence_stack.astype(jnp.float32)
    normed = (
        normalize(incoming_sequence_stack).astype(jnp.bfloat16).reshape(-1, hidden_channel_size)
    )
    row_whole = lax.all_gather(horizontal_projection_triple, "rows", axis=1, tiled=True)
    packed = jnp.dot(normed, row_whole, preferred_element_type=jnp.float32)
    queries, key_rows, value_rows = split_three(
        packed, hidden_channel_size, head_count, sequences_per_shard, sequence_positions
    )
    partial_value = jnp.einsum(
        "rihe,rjhe->hij", queries, key_rows, preferred_element_type=jnp.float32
    )
    bias_own = jnp.dot(
        twofold_contacts.reshape(-1, channels),
        contact_logit_offsets,
        preferred_element_type=jnp.float32,
    )
    bias_own = bias_own.reshape(residue_portion, sequence_positions, head_count).transpose(2, 0, 1)
    owned = lax.psum_scatter(partial_value, "rows", scatter_dimension=1, tiled=True)
    scores = owned * scale_rows + bias_own
    probs_own = masked_softmax(scores, protein_spans)
    row_probs = lax.all_gather(probs_own, "rows", axis=1, tiled=True)
    flat_scores = scores.astype(jnp.bfloat16).transpose(1, 2, 0).reshape(-1, head_count)
    pair_feature_output = (
        twofold_contacts.astype(jnp.float32)
        + jnp.dot(
            flat_scores, contact_projection_weights, preferred_element_type=jnp.float32
        ).reshape(residue_portion, sequence_positions, channels)
    ).astype(jnp.bfloat16)
    blended = jnp.einsum(
        "hij,rjhe->rihe", row_probs, value_rows, preferred_element_type=jnp.float32
    )
    blended = blended.astype(jnp.bfloat16).reshape(-1, hidden_channel_size)
    out_whole = lax.all_gather(horizontal_projection_out, "rows", axis=1, tiled=True)
    attended = jnp.dot(blended, out_whole, preferred_element_type=jnp.float32)
    updated_alignment = (
        incoming_sequence_stack
        + attended.reshape(sequences_per_shard, sequence_positions, hidden_channel_size)
    ).astype(jnp.bfloat16)
    columns = lax.all_to_all(updated_alignment, "rows", split_axis=1, concat_axis=0, tiled=True)
    column_input_rows = columns.astype(jnp.float32)
    col_normed = normalize(column_input_rows).astype(jnp.bfloat16).reshape(-1, hidden_channel_size)
    col_whole = lax.all_gather(vertical_projection_triple, "rows", axis=1, tiled=True)
    col_packed = jnp.dot(col_normed, col_whole, preferred_element_type=jnp.float32)
    col_queries, col_keys, col_values = split_three(
        col_packed, hidden_channel_size, head_count, overall_sequence_number, residue_portion
    )
    logits = jnp.einsum(
        "alhe,blhe->lhab", col_queries, col_keys, preferred_element_type=jnp.float32
    )
    col_probs = jax.nn.softmax(logits, axis=-1).astype(jnp.bfloat16)
    column_mixed_output = jnp.einsum(
        "lhab,blhe->alhe", col_probs, col_values, preferred_element_type=jnp.float32
    )
    column_mixed_output = column_mixed_output.astype(jnp.bfloat16).reshape(-1, hidden_channel_size)
    col_out_whole = lax.all_gather(vertical_projection_out, "rows", axis=1, tiled=True)
    column_attention_result = jnp.dot(
        column_mixed_output, col_out_whole, preferred_element_type=jnp.float32
    )
    alignment_output = (
        column_input_rows
        + column_attention_result.reshape(
            overall_sequence_number, residue_portion, hidden_channel_size
        )
    ).astype(jnp.bfloat16)
    return (alignment_output, pair_feature_output)


LANES = 128
BF = jnp.bfloat16
F32 = jnp.float32


def iota(shape, axis):
    return lax.broadcasted_iota(jnp.int32, shape, axis)


def dot(a, b, ca=1, cb=0, precision=None):
    return lax.dot_general(
        a, b, (((ca,), (cb,)), ((), ())), preferred_element_type=F32, precision=precision
    )


def exchange_partner(me, k, n):
    at, bit = me, 1
    while bit < n:
        if k & bit:
            at = at + bit * (1 - 2 * lax.rem(me // bit, 2))
        bit *= 2
    return at


def gathered_tile(slabs, width, tile):
    total = None
    for d in range(slabs.shape[0]):
        first = (width * d) // LANES
        last = (width * (d + 1) - 1) // LANES
        if first <= tile <= last:
            at = (tile - first) * LANES
            piece = slabs[d, :, at : at + LANES]
            total = piece if total is None else total + piece
    return total


def fused_kernel(
    n,
    copies,
    cuts,
    head_dim,
    seq_hbm,
    span_ref,
    con_hbm,
    offs_hbm,
    cw_hbm,
    w1_hbm,
    o1_hbm,
    w2_hbm,
    o2_hbm,
    out_ref,
    pair_ref,
    w1,
    o1,
    w2,
    seq_all,
    pk1,
    up_all,
    pk2,
    got,
    o2_all,
    offs_ref,
    cw_ref,
    load_sem,
    send_sem,
    recv_sem,
):
    me = lax.axis_index("rows")
    peers = [exchange_partner(me, k, n) for k in range(n)]
    order = list(range(n - 1, 0, -1))
    mine_a = lax.axis_index("aln")
    twins = [exchange_partner(mine_a, q, copies) for q in range(copies)]
    far_first = [k for k in order if k % 2 == 0]
    near_first = far_first[::-1]
    other = peers[1]
    length, width_d = seq_hbm.shape
    heads, channels = offs_ref.shape
    w_cols = w1_hbm.shape[0]
    o_cols = o1_hbm.shape[0]
    shift = pl.multiple_of(lax.rem(w_cols * me, LANES), 16)

    loads = [
        pltpu.make_async_copy(src, dst, load_sem.at[s])
        for s, (src, dst) in enumerate((
            (w1_hbm, w1.at[pl.ds(shift, w_cols)]),
            (o1_hbm, o1),
            (w2_hbm, w2.at[pl.ds(shift, w_cols)]),
            (o2_hbm, o2_all.at[me]),
            (seq_hbm, seq_all.at[me, :, pl.ds(0, width_d)]),
            (con_hbm, seq_all.at[me, :, pl.ds(width_d, channels)]),
            (offs_hbm, offs_ref),
            (cw_hbm, cw_ref),
        ))
    ]
    barrier = pltpu.get_barrier_semaphore()
    for k in order:
        pl.semaphore_signal(
            barrier, inc=1, device_id={"rows": peers[k]}, device_id_type=pl.DeviceIdType.MESH
        )
    for q in range(1, copies):
        pl.semaphore_signal(
            barrier,
            inc=1,
            device_id={"aln": twins[q], "rows": me},
            device_id_type=pl.DeviceIdType.MESH,
        )
    loads[4].start()
    loads[5].start()
    w1[...] = jnp.zeros_like(w1)
    w2[...] = jnp.zeros_like(w2)
    for c in loads[:4] + loads[6:]:
        c.start()
    loads[4].wait()
    loads[5].wait()
    pl.semaphore_wait(barrier, n - 1 + copies - 1)

    def send(phase, sem, k, src, dst, to=None, twin=0):
        pltpu.make_async_remote_copy(
            src_ref=src,
            dst_ref=dst,
            send_sem=send_sem.at[phase],
            recv_sem=recv_sem.at[sem],
            device_id={"aln": twins[twin], "rows": peers[k] if to is None else to},
            device_id_type=pl.DeviceIdType.MESH,
        ).start()

    def finish(phase, ref):
        pltpu.make_async_remote_copy(
            src_ref=ref,
            dst_ref=ref,
            send_sem=send_sem.at[phase],
            recv_sem=recv_sem.at[0],
            device_id={"rows": other},
            device_id_type=pl.DeviceIdType.MESH,
        ).wait_send()

    def receive(sem, ref):
        pltpu.make_async_remote_copy(
            src_ref=ref,
            dst_ref=ref,
            send_sem=send_sem.at[0],
            recv_sem=recv_sem.at[sem],
            device_id={"rows": other},
            device_id_type=pl.DeviceIdType.MESH,
        ).wait_recv()

    half = n // 2
    AT_X, AT_A2A = 0, 1
    AT_PK, AT_UP, AT_CUT, AT_TWIN = (2 + half * q for q in range(4))

    rows_c = o_cols // cuts[0]
    lanes_c = o2_hbm.shape[1] // cuts[1]

    def cut(slab, share):
        top = pl.multiple_of(share // cuts[1] * rows_c, rows_c)
        left = pl.multiple_of(lax.rem(share, cuts[1]) * lanes_c, lanes_c)
        return o2_all.at[slab, pl.ds(top, rows_c), pl.ds(left, lanes_c)]

    def spread(phase, at, slabs):
        for k in far_first:
            send(phase, at + k // 2, k, slabs.at[me], slabs.at[me])
        send(phase, at, 1, slabs.at[me], slabs.at[me])

    def collect(phase, at, slabs):
        for k in near_first:
            receive(at + k // 2, slabs.at[peers[k]])
            send(phase, at, k + 1, slabs.at[peers[k]], slabs.at[peers[k]], other)
        receive(at, slabs.at[pl.ds(0, half)])

    for k in order:
        send(0, AT_X, k, seq_all.at[me], seq_all.at[me])
    loads[3].wait()
    share = cut(me, mine_a)
    for k in far_first:
        send(4, AT_CUT + k // 2, k, share, share)
    send(4, AT_CUT, 1, o2_all.at[me], o2_all.at[me])

    tokens = n * length
    per_tile = LANES // head_dim
    tiles = width_d // LANES
    hi = heads * length

    tok_r = iota((tokens, tokens), 0) // length
    tok_i = iota((tokens, tokens), 0) % length
    lane_r = iota((tokens, tokens), 1) // length
    lane_i = iota((tokens, tokens), 1) % length
    same_r = tok_r == lane_r
    same_i = tok_i == lane_i
    fold = jnp.where(same_i, 1.0, 0.0).astype(F32)
    lane = iota((tokens, LANES), 1)

    def split_heads(tile):
        f = tile.astype(F32)
        return jnp.concatenate(
            [
                jnp.where((lane >= s * head_dim) & (lane < (s + 1) * head_dim), f, 0.0)
                for s in range(per_tile)
            ],
            axis=0,
        ).astype(BF)

    def join_heads(stack):
        total = stack[:tokens]
        for s in range(1, per_tile):
            total = jnp.where(lane >= s * head_dim, stack[s * tokens : (s + 1) * tokens], total)
        return total

    def project(x, w, slot):
        slot[me] = dot(x, w[...], 1, 1).astype(BF)

    rows_f = [None] * n
    loads[6].wait()
    loads[7].wait()
    pick = jnp.where(iota((hi, heads), 0) // length == iota((hi, heads), 1), 1.0, 0.0)
    offs_rep = dot(pick.astype(BF), offs_ref[...]).astype(BF)
    mine = jnp.where(iota((hi, heads), 0) % length == me, pick, 0.0).astype(BF)
    cw_rep = dot(mine, cw_ref[...]).astype(BF)
    columns = iota((o_cols, width_d), 1) == iota((o_cols, width_d), 0) + o_cols * me
    columns = jnp.where(columns, 1.0, 0.0).astype(BF)

    receive(AT_X, seq_all.at[pl.ds(0, n - 1)])
    x = seq_all[:, :, :width_d].astype(F32).reshape(tokens, width_d)
    x_own = dot(x.astype(BF), columns, 1, 1)
    normed = normalize(x).astype(BF)
    loads[0].wait()
    project(normed, w1, pk1)
    spread(1, AT_PK, pk1)
    for k in near_first:
        share = cut(peers[k], mine_a)
        receive(AT_CUT + k // 2, share)
        for q in range(1, copies):
            send(4, AT_TWIN + k // 2, k, share, share, me, q)
    con = seq_all[:, :, width_d:].astype(F32).reshape(tokens, channels).astype(BF)
    bias = dot(offs_rep, con, 1, 1)
    own = iota((hi, tokens), 0) % length == iota((hi, tokens), 1) // length
    bias = jnp.where(own, bias, 0.0)
    collect(1, AT_PK, pk1)
    tied = []
    for t in range(tiles):
        q = split_heads(gathered_tile(pk1, w_cols, t))
        kk = gathered_tile(pk1, w_cols, tiles + t)
        s = dot(q, kk, 1, 1).reshape(per_tile, tokens, tokens)
        s = jnp.where(same_r[None], s, 0.0).reshape(per_tile, n, length, tokens)
        tied.append(jnp.sum(s, axis=1).reshape(per_tile * length, tokens))
    tied = jnp.concatenate(tied, axis=0)
    scale = head_dim ** (-0.5) * float(n) ** (-0.5)
    scores = dot(tied * scale + bias, fold, precision=lax.Precision.HIGHEST)

    key_ok = iota((hi, tokens), 1) % length < span_ref[0]
    logits = jnp.where(key_ok, scores, -1e30)
    e = jnp.exp(logits - jnp.max(logits, axis=1, keepdims=True))
    probs = e / (jnp.sum(e, axis=1, keepdims=True) * (1.0 / n))
    probs = probs.astype(BF).astype(F32)
    blended = []
    for t in range(tiles):
        rows = per_tile * length
        p = probs[t * rows : (t + 1) * rows].reshape(per_tile, 1, length, tokens)
        p = jnp.broadcast_to(p, (per_tile, n, length, tokens)).reshape(per_tile, tokens, tokens)
        p = jnp.where(same_r[None], p, 0.0).reshape(per_tile * tokens, tokens).astype(BF)
        v = gathered_tile(pk1, w_cols, 2 * tiles + t)
        blended.append(join_heads(dot(p, v)).astype(BF))
    blended = jnp.concatenate(blended, axis=1)
    loads[1].wait()
    up_all[me, :, :o_cols] = (x_own + dot(blended, o1[...], 1, 1)).astype(BF)
    spread(2, AT_UP, up_all)
    for k in near_first:
        receive(AT_TWIN + k // 2, cut(pl.ds(0, copies - 1), 0))
        send(4, AT_CUT, k + 1, o2_all.at[peers[k]], o2_all.at[peers[k]], other)

    add = dot(scores.astype(BF), cw_rep, 0, 0)[:length]
    pair_ref[...] = (seq_all[me, :, width_d:].astype(F32) + add).astype(BF)

    collect(2, AT_UP, up_all)
    updated = jnp.concatenate(
        [up_all[d].astype(F32)[:, :o_cols] for d in range(n)], axis=1
    )
    perm = jnp.where((tok_r == lane_i) & (tok_i == lane_r), 1.0, 0.0).astype(BF)
    normed = dot(perm, normalize(updated).astype(BF)).astype(BF)
    loads[2].wait()
    pk2[...] = dot(normed, w2[...], 1, 1).reshape(length, n, w2.shape[0]).astype(BF)
    for k in order:
        send(3, AT_A2A, k, pk2.at[peers[k]], got.at[me])
    got[me] = pk2[me]
    sel = (iota((n, tokens), 0) == iota((n, tokens), 1) // length) & (
        iota((n, tokens), 1) % length == me
    )
    residual = dot(jnp.where(sel, 1.0, 0.0).astype(BF), updated.astype(BF))
    receive(AT_A2A, got.at[pl.ds(0, n - 1)])
    lane_n = iota((n, LANES), 1)
    mixed = []
    for t in range(tiles):
        qf = gathered_tile(got, w_cols, t).astype(F32)
        q = jnp.concatenate(
            [
                jnp.where((lane_n >= h * head_dim) & (lane_n < (h + 1) * head_dim), qf, 0.0)
                for h in range(per_tile)
            ],
            axis=0,
        ).astype(BF)
        kk = gathered_tile(got, w_cols, tiles + t)
        s = dot(q, kk, 1, 1) * head_dim ** (-0.5)
        e = jnp.exp(s - jnp.max(s, axis=1, keepdims=True))
        p = (e / jnp.sum(e, axis=1, keepdims=True)).astype(BF)
        both = dot(p, gathered_tile(got, w_cols, 2 * tiles + t))
        total = both[:n]
        for h in range(1, per_tile):
            total = jnp.where(lane_n >= h * head_dim, both[h * n : (h + 1) * n], total)
        mixed.append(total)
    mixed = jnp.concatenate(mixed, axis=1).astype(BF)
    receive(AT_CUT, o2_all.at[pl.ds(0, half)])
    final = jnp.concatenate(
        [dot(mixed, o2_all[d], 1, 1) for d in range(n)], axis=1
    )
    out_ref[...] = (residual + final).astype(BF)
    for phase, slabs in enumerate((seq_all, pk1, up_all, got, o2_all)):
        finish(phase, slabs.at[pl.ds(0, n - 1)])


def emit_kernel(out_ref, pair_ref, out_hbm, pair_hbm, sem):
    copies = [
        pltpu.make_async_copy(src, dst, sem.at[at])
        for at, (src, dst) in enumerate(((out_ref, out_hbm), (pair_ref, pair_hbm)))
    ]
    for c in copies:
        c.start()
    for c in copies:
        c.wait()


def fused_device(n, copies, cuts, seq, spans, con, w1, o1, w2, o2, offs, cw):
    _, length, width = seq.shape
    channels, heads = offs.shape
    w1, o1, w2, o2, offs = w1.T, o1.T, w2.T, o2.T, offs.T
    tokens = n * length
    window = max(
        -(-((w1.shape[0] * d) % LANES + w1.shape[0]) // LANES) for d in range(n)
    ) * LANES
    o_window = -(-o1.shape[0] // LANES) * LANES
    vmem = pl.BlockSpec(memory_space=pltpu.VMEM)
    hbm = pl.BlockSpec(memory_space=pl.ANY)
    out, pair = pl.pallas_call(
        functools.partial(fused_kernel, n, copies, cuts, width // heads),
        out_shape=(pltpu.VMEM((n, width), BF), pltpu.VMEM((length, channels), BF)),
        in_specs=[hbm, pl.BlockSpec(memory_space=pltpu.SMEM), *[hbm] * 7],
        out_specs=(vmem, vmem),
        scratch_shapes=[
            pltpu.VMEM((window, width), BF),
            pltpu.VMEM(o1.shape, BF),
            pltpu.VMEM((window, width), BF),
            pltpu.VMEM((n, length, width + channels), BF),
            pltpu.VMEM((n, tokens, window), BF),
            pltpu.VMEM((n, tokens, o_window), BF),
            pltpu.VMEM((length, n, window), BF),
            pltpu.VMEM((n, n, window), BF),
            pltpu.VMEM((n, *o2.shape), BF),
            pltpu.VMEM(offs.shape, BF),
            pltpu.VMEM(cw.shape, BF),
            pltpu.SemaphoreType.DMA((8,)),
            pltpu.SemaphoreType.DMA((5,)),
            pltpu.SemaphoreType.DMA((2 + 4 * (n // 2),)),
        ],
        compiler_params=pltpu.CompilerParams(collective_id=0, has_side_effects=True),
    )(seq.reshape(length, width), spans, con.reshape(length, channels), offs, cw, w1, o1, w2, o2)
    out, pair = (pltpu.with_memory_space_constraint(a, pltpu.VMEM) for a in (out, pair))
    out, pair = pl.pallas_call(
        emit_kernel,
        out_shape=(
            jax.ShapeDtypeStruct((n, width), BF),
            jax.ShapeDtypeStruct((length, channels), BF),
        ),
        in_specs=[vmem, vmem],
        out_specs=(hbm, hbm),
        scratch_shapes=[pltpu.SemaphoreType.DMA((2,))],
    )(out, pair)
    return out.reshape(n, 1, width), pair.reshape(1, length, channels)


def dispatch(n, copies, *args):
    seq, _, con, w1, o1 = args[:5]
    heads = args[7].shape[1]
    rows, length, width = seq.shape
    head_dim = width // heads
    fits = (
        rows == 1
        and con.shape[0] == 1
        and length == n
        and n % 8 == 0
        and n & (n - 1) == 0
        and w1.shape[1] % 16 == 0
        and n * length <= 256
        and width % LANES == 0
        and LANES % head_dim == 0
    )
    cuts = [
        (down, copies // down)
        for down in range(1, copies + 1)
        if copies % down == 0
        and args[4].shape[1] % (16 * down) == 0
        and width % (LANES * (copies // down)) == 0
    ]
    if fits and copies & (copies - 1) == 0 and cuts:
        return fused_device(n, copies, cuts[-1], *args)
    return per_device(*args)


def solution(mesh):
    placed = (
        P(("aln", "rows"), None, None),
        P("aln"),
        P(("aln", "rows"), None, None),
        P(None, "rows"),
        P(None, "rows"),
        P(None, "rows"),
        P(None, "rows"),
        P(),
        P(),
    )
    return jax.shard_map(
        functools.partial(dispatch, mesh.shape["rows"], mesh.shape["aln"]),
        mesh=mesh,
        in_specs=placed,
        out_specs=(P("aln", "rows", None), P(("aln", "rows"), None, None)),
        check_vma=False,
    )
```
